32 devices in a mesh: band: 8 (over z, y), grid: 4 (over x, core).
Axes of the slice: x: 2, y: 2, z: 4, core: 2. Of those that a mesh axis runs over, the one named last changes fastest.
Arguments:
- own_bands: float32 [32, 128, 128, 128], P('band', 'grid'), may hold values from -1.5 to 1.5
- travel_bands: float32 [32, 128, 128, 128], P('band', 'grid'), may hold values from -1.5 to 1.5
Outputs:
- own_terms: float32 [32, 128, 128, 128], P('band', 'grid')
- partner_terms: float32 [32, 128, 128, 128], P('band', 'grid')
The draws below stay inside these ranges and needn't reach their ends.
All inputs are finite; a program needn't handle non-finite values.
Results may differ from the reference program's by a relative error of at most 0.00011.
Values sent between devices are 32-bit elements; how exact they have to be, the bound alone decides.
No kernel may reach another device: no remote copies, remote signals or barrier semaphores. Data moves between devices by JAX's collectives and lax.ppermute only.
A program may use at most 192 MiB of HBM per device.

```python
import math
import jax
import jax.numpy as jnp
from jax import lax

NX = 128
NY = 128
NZ = 128
OWN = 4
VIS = 4
BANDS = 32
TRAVEL = 32
N_BAND = 8


def band_field(base_key, band_count):
    return 0.5 * jax.random.truncated_normal(jax.random.fold_in(base_key, 4), -3.0, 3.0, (band_count, NZ, NY, NX), jnp.float32)


def draw_own_bands(key, part):
    return band_field(jax.random.fold_in(key, 11), BANDS)


def draw_travel_bands(key, part):
    return band_field(jax.random.fold_in(key, 23), TRAVEL)


def setup_inputs(seed: int = 0) -> dict:
    streams_of = jax.random.split(jax.random.key(seed), 3)
    return {
        "own_bands": draw_own_bands(jax.random.fold_in(streams_of[2], 71), 0),
        "travel_bands": draw_travel_bands(jax.random.fold_in(streams_of[2], 71), 0),
    }


FRACTION = 0.25


def wave_square(points, first_row, length):
    position = first_row + jnp.arange(points, dtype=jnp.int32)
    position = (position + length // 2) % length - length // 2
    wavenumber = (2.0 * math.pi / length) * position.astype(jnp.float32)
    return wavenumber * wavenumber


def coulomb(first_row, row_count):
    squared = wave_square(NZ, 0, NZ)[:, None, None] + wave_square(row_count, first_row, NY)[None, :, None] + wave_square(NX, 0, NX)[None, None, :]
    safe_square = jnp.where(squared > 0.0, squared, 1.0)
    return jnp.where(squared > 0.0, 4.0 * math.pi / safe_square, 0.0)


def reference(own_bands, travel_bands):
    kernel = coulomb(0, NY)[:, :, : NX // 2 + 1]
    owned_groups = own_bands.reshape(N_BAND, OWN, NZ, NY, NX)
    arrived = jnp.roll(travel_bands.reshape(N_BAND, VIS, NZ, NY, NX), 1, axis=0)

    def group_terms(blocks):
        owned, visitors = blocks

        def visit_band(accumulated, visitor):
            density = owned * visitor
            potential = jnp.fft.irfftn(kernel * jnp.fft.rfftn(density, axes=(1, 2, 3)), s=(NZ, NY, NX), axes=(1, 2, 3))
            return accumulated + potential * visitor, jnp.sum(potential * owned, axis=0)

        accumulated, partner = lax.scan(visit_band, jnp.zeros_like(owned), visitors)
        return -FRACTION * accumulated, -FRACTION * partner

    own_terms, held = lax.map(group_terms, (owned_groups, arrived))
    held = jnp.roll(held, -1, axis=0)
    return own_terms.reshape(BANDS, NZ, NY, NX), held.reshape(TRAVEL, NZ, NY, NX)
```

```python
import math, functools
import numpy as np
import jax
import jax.numpy as jnp
from jax import lax
from jax.experimental import pallas as pl
from jax.experimental.pallas import tpu as pltpu
import ml_dtypes
BF = jnp.bfloat16
F32 = jnp.float32

def split_table(t):
    hi = t.astype(np.float32).astype(ml_dtypes.bfloat16)
    lo = (t - hi.astype(np.float64)).astype(np.float32).astype(ml_dtypes.bfloat16)
    return hi, lo

def dft(length, inverse):
    k = np.arange(length)
    ang = 2.0 * np.pi / length * ((k[:, None] * k[None, :]) % length)
    c, s = np.cos(ang), np.sin(ang)
    if inverse:
        s = -s
    return np.block([[c, s], [-s, c]])

def left_table(length, inverse):
    hi, lo = split_table(dft(length, inverse))
    return np.concatenate([hi, hi, lo], axis=1)

def right_table(length, inverse):
    hi, lo = split_table(dft(length, inverse).T)
    return np.concatenate([hi, hi, lo], axis=0)

def parts(v):
    hi = v.astype(BF)
    lo = (v - hi.astype(F32)).astype(BF)
    return hi, lo

def fft_body(*refs, n, pz, py, chunk, pitch, accumulate, n_own, four_pi):
    nz, ny, nx = n
    (q_ref, own_ref, vis_ref) = refs[:3]
    rest = list(refs[3:])
    prev_ref = rest.pop(0) if accumulate else None
    lyf, lyi, rxf, rxi, lzf, lzi, own_out, part_out, re_s, im_s, st_l, st_r, st_z, st_z2, ksq = rest
    step = pl.program_id(0)
    na = nz // pz
    nb = ny // py

    def put_left(st, a, j, w, re, im):
        rh, rl = parts(re); ih, il = parts(im)
        col = slice(j * w, (j + 1) * w)
        st[0 * a:1 * a, col] = rh
        st[1 * a:2 * a, col] = ih
        st[2 * a:3 * a, col] = rl
        st[3 * a:4 * a, col] = il
        st[4 * a:5 * a, col] = rh
        st[5 * a:6 * a, col] = ih

    def put_right(st, a, w, j, re, im):
        rh, rl = parts(re); ih, il = parts(im)
        row = slice(j * a, (j + 1) * a)
        st[row, 0 * w:1 * w] = rh
        st[row, 1 * w:2 * w] = ih
        st[row, 2 * w:3 * w] = rl
        st[row, 3 * w:4 * w] = il
        st[row, 4 * w:5 * w] = rh
        st[row, 5 * w:6 * w] = ih

    def dot(a, b):
        return lax.dot_general(a, b, (((1,), (0,)), ((), ())), preferred_element_type=F32)

    @pl.when(step < na)
    def _():
        z0 = step * pz
        for c0 in range(0, pz, chunk):
            for p in range(c0, c0 + chunk):
                v = vis_ref[p]
                re = own_ref[0, p] * v
                im = own_ref[1, p] * v if n_own == 2 else jnp.zeros_like(re)
                put_left(st_l, ny, p, nx, re, im)
            y1 = dot(lyf[...], st_l[:, c0 * nx:(c0 + chunk) * nx])
            for p in range(c0, c0 + chunk):
                j = p - c0
                put_right(st_r, ny, nx, p, y1[:ny, j * nx:(j + 1) * nx], y1[ny:, j * nx:(j + 1) * nx])
            y2 = dot(st_r[c0 * ny:(c0 + chunk) * ny, :], rxf[...])
            for p in range(c0, c0 + chunk):
                j = p - c0
                row = pl.multiple_of((z0 + p) * pitch, 8)
                re_s[pl.ds(row, ny), :] = y2[j * ny:(j + 1) * ny, :nx]
                im_s[pl.ds(row, ny), :] = y2[j * ny:(j + 1) * ny, nx:]

    def square(i, length):
        pos = jnp.where(i >= length // 2, i - length, i).astype(F32) * F32(2.0 * math.pi / length)
        return pos * pos

    @pl.when(step == na)
    def _():
        iz = lax.broadcasted_iota(jnp.int32, (nz, nx), 0)
        ix = lax.broadcasted_iota(jnp.int32, (nz, nx), 1)
        ksq[...] = square(iz, nz) + square(ix, nx)

    @pl.when((step >= na) & (step < na + nb))
    def _():
        y0 = (step - na) * py
        for c0 in range(0, py, chunk):
            for j in range(c0, c0 + chunk):
                re = re_s[pl.ds(y0 + j, nz, stride=pitch), :]
                im = im_s[pl.ds(y0 + j, nz, stride=pitch), :]
                put_left(st_z, nz, j, nx, re, im)
            f = dot(lzf[...], st_z[:, c0 * nx:(c0 + chunk) * nx])
            for j in range(c0, c0 + chunk):
                k2 = ksq[...] + square(y0 + j, ny)
                kern = jnp.where(k2 > 0.0, F32(four_pi) / jnp.where(k2 > 0.0, k2, 1.0), 0.0)
                i = j - c0
                put_left(st_z2, nz, j, nx, f[:nz, i * nx:(i + 1) * nx] * kern, f[nz:, i * nx:(i + 1) * nx] * kern)
            g = dot(lzi[...], st_z2[:, c0 * nx:(c0 + chunk) * nx])
            for j in range(c0, c0 + chunk):
                i = j - c0
                re_s[pl.ds(y0 + j, nz, stride=pitch), :] = g[:nz, i * nx:(i + 1) * nx]
                im_s[pl.ds(y0 + j, nz, stride=pitch), :] = g[nz:, i * nx:(i + 1) * nx]

    @pl.when(step >= na + nb)
    def _():
        z0 = (step - na - nb) * pz
        for c0 in range(0, pz, chunk):
            for p in range(c0, c0 + chunk):
                row = pl.multiple_of((z0 + p) * pitch, 8)
                put_right(st_r, ny, nx, p, re_s[pl.ds(row, ny), :], im_s[pl.ds(row, ny), :])
            y2 = dot(st_r[c0 * ny:(c0 + chunk) * ny, :], rxi[...])
            for p in range(c0, c0 + chunk):
                j = p - c0
                put_left(st_l, ny, p, nx, y2[j * ny:(j + 1) * ny, :nx], y2[j * ny:(j + 1) * ny, nx:])
            y1 = dot(lyi[...], st_l[:, c0 * nx:(c0 + chunk) * nx])
            for p in range(c0, c0 + chunk):
                j = p - c0
                v = vis_ref[p]
                va = y1[:ny, j * nx:(j + 1) * nx]
                o = va * v
                own_out[0, p] = o + prev_ref[0, p] if accumulate else o
                pt = va * own_ref[0, p]
                if n_own == 2:
                    vb = y1[ny:, j * nx:(j + 1) * nx]
                    o = vb * v
                    own_out[1, p] = o + prev_ref[1, p] if accumulate else o
                    pt = pt + vb * own_ref[1, p]
                part_out[p] = pt

def solve(q, own, vis, prev, pieces, scale, pz=8, py=8, chunk=2, pad=8):
    n_own, nz, ny, nx = own.shape
    a, b = pieces
    planes = nz // (a * b)
    na, nb = nz // pz, ny // py
    per = planes // pz

    def zblk(i, q):
        t = jnp.where(i < na, i, jnp.maximum(i - nb, na) - na)
        t = jnp.where((i >= na) & (i < na + nb), na - 1, t)
        piece = t // per
        x, c = piece // b, piece % b
        rel = ((x - q[0] + a) % a) * b + (c - q[1] + b) % b
        return rel * per + t % per

    def zout(i, q):
        t = jnp.maximum(i - nb - na, 0)
        piece = t // per
        x, c = piece // b, piece % b
        rel = ((x - q[0] + a) % a) * b + (c - q[1] + b) % b
        return rel * per + t % per

    own_in = pl.BlockSpec((n_own, pz, ny, nx), lambda i, q: (0, zblk(i, q), 0, 0))
    vis_in = pl.BlockSpec((pz, ny, nx), lambda i, q: (zblk(i, q), 0, 0))
    prev_in = pl.BlockSpec((n_own, pz, ny, nx), lambda i, q: (0, zout(i, q), 0, 0))
    own_o = pl.BlockSpec((n_own, pz, ny, nx), lambda i, q: (0, zout(i, q), 0, 0))
    part_o = pl.BlockSpec((pz, ny, nx), lambda i, q: (zout(i, q), 0, 0))
    tabs = [left_table(ny, False), left_table(ny, True), right_table(nx, False), right_table(nx, True), left_table(nz, False), left_table(nz, True)]
    tab_specs = [pl.BlockSpec(t.shape, lambda i, q: (0, 0)) for t in tabs]
    pitch = ny + pad
    body = functools.partial(fft_body, n=(nz, ny, nx), pz=pz, py=py, chunk=chunk, pitch=pitch, accumulate=prev is not None, n_own=n_own, four_pi=scale)
    ins = [own, vis] + ([prev] if prev is not None else []) + [jnp.asarray(t) for t in tabs]
    specs = [own_in, vis_in] + ([prev_in] if prev is not None else []) + tab_specs
    flops = 6 * 3 * 2 * nz * ny * 4 * nx * nx
    return pl.pallas_call(
        body,
        grid_spec=pltpu.PrefetchScalarGridSpec(
            num_scalar_prefetch=1, grid=(2 * na + nb,), in_specs=specs, out_specs=[own_o, part_o],
            scratch_shapes=[pltpu.VMEM((nz * pitch, nx), F32), pltpu.VMEM((nz * pitch, nx), F32),
                            pltpu.VMEM((6 * ny, pz * nx), BF), pltpu.VMEM((pz * ny, 6 * nx), BF),
                            pltpu.VMEM((6 * nz, py * nx), BF), pltpu.VMEM((6 * nz, py * nx), BF),
                            pltpu.VMEM((nz, nx), F32)]),
        out_shape=[jax.ShapeDtypeStruct(own.shape, F32), jax.ShapeDtypeStruct(vis.shape, F32)],
        compiler_params=pltpu.CompilerParams(vmem_limit_bytes=56 * 2**20),
        cost_estimate=pl.CostEstimate(flops=flops, bytes_accessed=64 * 2**20, transcendentals=0),
    )(q, *ins)


from jax.sharding import PartitionSpec as P

FRACTION = 0.25


def factors(size, own, vis):
    pairs = [(a, size // a) for a in range(1, size + 1) if size % a == 0]
    return min((p for p in pairs if own % p[0] == 0 and vis % p[1] == 0), key=lambda p: abs(p[0] - p[1]))


def from_slow(block, a, b, shift):
    if shift == 0:
        return block
    return lax.ppermute(block, "grid", [(((x + shift) % a) * b + c, x * b + c) for x in range(a) for c in range(b)])


def from_fast(block, a, b, shift):
    if shift == 0:
        return block
    return lax.ppermute(block, "grid", [(x * b + (c + shift) % b, x * b + c) for x in range(a) for c in range(b)])


def along_band(block, distance):
    size = lax.axis_size("band")
    return lax.ppermute(block, "band", [((i - distance) % size, i) for i in range(size)])


def body(own_bands, travel_bands):
    own_count, planes, ny, nx = own_bands.shape
    vis_count = travel_bands.shape[0]
    size = lax.axis_size("grid")
    a, b = factors(size, own_count, vis_count)
    n_own, n_vis = own_count // a, vis_count // b
    nz = planes * size
    index = lax.axis_index("grid")
    x, c = index // b, index % b
    q = jnp.stack([x, c]).astype(jnp.int32)
    scale = -FRACTION * 4.0 * math.pi / (nz * ny * nx)
    pz = math.gcd(planes, 16)
    py = math.gcd(ny, 16)

    def own_set(s):
        return lax.dynamic_slice_in_dim(own_bands, s * n_own, n_own, 0)

    halves = []
    for k in range(n_vis):
        quarters = []
        for dc in range(b):
            piece = lax.dynamic_slice_in_dim(travel_bands, ((c - dc) % b) * n_vis + k, 1, 0)
            quarters.append(from_fast(piece, a, b, dc))
        halves.append(along_band(jnp.concatenate(quarters, axis=0), 1))

    own_x = [from_slow(own_set((x - dx) % a), a, b, dx) for dx in range(a)]
    own_half = jnp.stack(own_x, axis=1)
    own_full = jnp.stack([from_fast(own_half, a, b, dc) for dc in range(b)], axis=2)
    own_full = own_full.reshape(n_own, nz, ny, nx)

    groups = [(g, min(2, n_own - g)) for g in range(0, n_own, 2)]
    own_part = [None for _ in groups]
    partner_halves = []
    for k in range(n_vis):
        vis_full = jnp.concatenate([from_slow(halves[k], a, b, dx) for dx in range(a)], axis=0)
        vis_full = vis_full.reshape(nz, ny, nx)
        partner = None
        for n, (g, w) in enumerate(groups):
            own_part[n], part = solve(q, own_full[g:g + w], vis_full, own_part[n], (a, b), scale, pz=pz, py=py)
            partner = part if partner is None else partner + part
        partner = partner.reshape(a, b, planes, ny, nx)
        summed = None
        for dx in range(a):
            got = from_slow(partner[dx], a, b, (-dx) % a)
            summed = got if summed is None else summed + got
        partner_halves.append(along_band(summed, -1))

    own_part = (own_part[0] if len(groups) == 1 else jnp.concatenate(own_part, axis=0)).reshape(n_own, a, b, planes, ny, nx)
    summed = None
    for dc in range(b):
        got = from_fast(own_part[:, :, dc], a, b, (-dc) % b)
        summed = got if summed is None else summed + got
    own_out = jnp.zeros_like(own_bands)
    for dx in range(a):
        got = from_slow(summed[:, dx], a, b, (-dx) % a)
        own_out = lax.dynamic_update_slice_in_dim(own_out, got, ((x - dx) % a) * n_own, 0)
    partner_out = jnp.zeros_like(travel_bands)
    for k in range(n_vis):
        for dc in range(b):
            got = from_fast(partner_halves[k][dc:dc + 1], a, b, (-dc) % b)
            partner_out = lax.dynamic_update_slice_in_dim(partner_out, got, ((c - dc) % b) * n_vis + k, 0)
    return own_out, partner_out


def solution(mesh):
    spec = P("band", "grid", None, None)
    return jax.shard_map(body, mesh=mesh, in_specs=(spec, spec), out_specs=(spec, spec), check_vma=False)
```

```python
import math, functools
import numpy as np
import jax
import jax.numpy as jnp
from jax import lax
from jax.experimental import pallas as pl
from jax.experimental.pallas import tpu as pltpu
import ml_dtypes
BF = jnp.bfloat16
F32 = jnp.float32


def split_table(t):
    hi = t.astype(np.float32).astype(ml_dtypes.bfloat16)
    lo = (t - hi.astype(np.float64)).astype(np.float32).astype(ml_dtypes.bfloat16)
    return hi, lo


def dft(length, inverse):
    k = np.arange(length)
    ang = 2.0 * np.pi / length * ((k[:, None] * k[None, :]) % length)
    c, s = np.cos(ang), np.sin(ang)
    if inverse:
        s = -s
    return np.block([[c, s], [-s, c]])


def left_table(length, inverse):
    hi, lo = split_table(dft(length, inverse))
    return np.concatenate([hi, hi, lo], axis=1)


def right_table(length, inverse):
    hi, lo = split_table(dft(length, inverse).T)
    return np.concatenate([hi, hi, lo], axis=0)


def parts(v):
    hi = v.astype(BF)
    lo = (v - hi.astype(F32)).astype(BF)
    return hi, lo


def fft_body(*refs, n, pz, py, chunk, pitch, accumulate, n_own, four_pi, pieces, zchunk, lag):
    nz, ny, nx = n
    q_ref, own_ref = refs[:2]
    a, b = pieces
    vis_refs = refs[2:2 + a * b]
    rest = list(refs[2 + a * b:])
    prev_ref = rest.pop(0) if accumulate else None
    lyf, lyi, rxf, rxi, lzf, lzi, own_out, part_out, re_s, im_s, st_l, st_r, st_z2, ksq, vis_ref = rest
    st_z = st_l
    step = pl.program_id(0)
    na = nz // pz
    nb = ny // py

    def put_left(st, a, j, w, re, im):
        rh, rl = parts(re); ih, il = parts(im)
        col = slice(j * w, (j + 1) * w)
        st[0 * a:1 * a, col] = rh
        st[1 * a:2 * a, col] = ih
        st[2 * a:3 * a, col] = rl
        st[3 * a:4 * a, col] = il

    def put_right(st, a, w, j, re, im):
        rh, rl = parts(re); ih, il = parts(im)
        row = slice(j * a, (j + 1) * a)
        st[row, 0 * w:1 * w] = rh
        st[row, 1 * w:2 * w] = ih
        st[row, 2 * w:3 * w] = rl
        st[row, 3 * w:4 * w] = il

    def left(st, a, lo, hi):
        return jnp.concatenate([st[:4 * a, lo:hi], st[:2 * a, lo:hi]], axis=0)

    def right(st, w, lo, hi):
        return jnp.concatenate([st[lo:hi, :], st[lo:hi, :2 * w]], axis=1)

    def dot(a, b):
        return lax.dot_general(a, b, (((1,), (0,)), ((), ())), preferred_element_type=F32)

    def pipeline(first, second, third, count, width):
        n = count // width
        for t in range(n + 2 * lag):
            if t < n:
                first(t * width)
            if 0 <= t - lag < n:
                second((t - lag) * width)
            if 0 <= t - 2 * lag < n:
                third((t - 2 * lag) * width)

    plane = jnp.where(step < na, step, step - na - nb)
    natural = plane // (na // (a * b))
    for dx in range(a):
        for dc in range(b):
            here = ((q_ref[0] + dx) % a) * b + (q_ref[1] + dc) % b

            @pl.when(((step < na) | (step >= na + nb)) & (natural == here))
            def _(dx=dx, dc=dc):
                vis_ref[...] = vis_refs[dx * b + dc][0]

    @pl.when(step < na)
    def _():
        z0 = step * pz

        def density(c0):
            for p in range(c0, c0 + chunk):
                v = vis_ref[p]
                re = own_ref[0, 0, p] * v
                im = own_ref[0, 1, p] * v if n_own == 2 else jnp.zeros_like(re)
                put_left(st_l, ny, p, nx, re, im)

        def yforward(c0):
            y1 = dot(lyf[...], left(st_l, ny, c0 * nx, (c0 + chunk) * nx))
            for p in range(c0, c0 + chunk):
                j = p - c0
                put_right(st_r, ny, nx, p, y1[:ny, j * nx:(j + 1) * nx], y1[ny:, j * nx:(j + 1) * nx])

        def xforward(c0):
            y2 = dot(right(st_r, nx, c0 * ny, (c0 + chunk) * ny), rxf[...])
            for p in range(c0, c0 + chunk):
                j = p - c0
                row = pl.multiple_of((z0 + p) * pitch, 8)
                re_s[pl.ds(row, ny), :] = y2[j * ny:(j + 1) * ny, :nx]
                im_s[pl.ds(row, ny), :] = y2[j * ny:(j + 1) * ny, nx:]

        pipeline(density, yforward, xforward, pz, chunk)

    def square(i, length):
        pos = jnp.where(i >= length // 2, i - length, i).astype(F32) * F32(2.0 * math.pi / length)
        return pos * pos

    @pl.when(step == na)
    def _():
        iz = lax.broadcasted_iota(jnp.int32, (nz, nx), 0)
        ix = lax.broadcasted_iota(jnp.int32, (nz, nx), 1)
        ksq[...] = square(iz, nz) + square(ix, nx)

    @pl.when((step >= na) & (step < na + nb))
    def _():
        y0 = (step - na) * py

        def zload(c0):
            for j in range(c0, c0 + zchunk):
                re = re_s[pl.ds(y0 + j, nz, stride=pitch), :]
                im = im_s[pl.ds(y0 + j, nz, stride=pitch), :]
                put_left(st_z, nz, j, nx, re, im)

        def zforward(c0):
            f = dot(lzf[...], left(st_z, nz, c0 * nx, (c0 + zchunk) * nx))
            for j in range(c0, c0 + zchunk):
                k2 = ksq[...] + square(y0 + j, ny)
                kern = jnp.where(k2 > 0.0, F32(four_pi) / jnp.where(k2 > 0.0, k2, 1.0), 0.0)
                i = j - c0
                put_left(st_z2, nz, j, nx, f[:nz, i * nx:(i + 1) * nx] * kern, f[nz:, i * nx:(i + 1) * nx] * kern)

        def zinverse(c0):
            g = dot(lzi[...], left(st_z2, nz, c0 * nx, (c0 + zchunk) * nx))
            for j in range(c0, c0 + zchunk):
                i = j - c0
                re_s[pl.ds(y0 + j, nz, stride=pitch), :] = g[:nz, i * nx:(i + 1) * nx]
                im_s[pl.ds(y0 + j, nz, stride=pitch), :] = g[nz:, i * nx:(i + 1) * nx]

        pipeline(zload, zforward, zinverse, py, zchunk)

    @pl.when(step >= na + nb)
    def _():
        z0 = (step - na - nb) * pz

        def spectrum(c0):
            for p in range(c0, c0 + chunk):
                row = pl.multiple_of((z0 + p) * pitch, 8)
                put_right(st_r, ny, nx, p, re_s[pl.ds(row, ny), :], im_s[pl.ds(row, ny), :])

        def xinverse(c0):
            y2 = dot(right(st_r, nx, c0 * ny, (c0 + chunk) * ny), rxi[...])
            for p in range(c0, c0 + chunk):
                j = p - c0
                put_left(st_l, ny, p, nx, y2[j * ny:(j + 1) * ny, :nx], y2[j * ny:(j + 1) * ny, nx:])

        def yinverse(c0):
            y1 = dot(lyi[...], left(st_l, ny, c0 * nx, (c0 + chunk) * nx))
            for p in range(c0, c0 + chunk):
                j = p - c0
                v = vis_ref[p]
                va = y1[:ny, j * nx:(j + 1) * nx]
                o = va * v
                own_out[0, 0, p] = o + prev_ref[0, 0, p] if accumulate else o
                pt = va * own_ref[0, 0, p]
                if n_own == 2:
                    vb = y1[ny:, j * nx:(j + 1) * nx]
                    o = vb * v
                    own_out[0, 1, p] = o + prev_ref[0, 1, p] if accumulate else o
                    pt = pt + vb * own_ref[0, 1, p]
                part_out[0, p] = pt

        pipeline(spectrum, xinverse, yinverse, pz, chunk)


def solve(q, own, vis, prev, pieces, scale, pz=8, py=8, chunk=2, pad=8, zchunk=None, lag=1):
    _, n_own, planes, ny, nx = own.shape
    a, b = pieces
    nz = planes * a * b
    na, nb = nz // pz, ny // py
    per = planes // pz

    def zblk(i, q):
        t = jnp.where(i < na, i, jnp.maximum(i - nb, na) - na)
        t = jnp.where((i >= na) & (i < na + nb), na - 1, t)
        piece = t // per
        x, c = piece // b, piece % b
        rel = ((x - q[0] + a) % a) * b + (c - q[1] + b) % b
        return rel, t % per

    def zout(i, q):
        t = jnp.maximum(i - nb - na, 0)
        piece = t // per
        x, c = piece // b, piece % b
        rel = ((x - q[0] + a) % a) * b + (c - q[1] + b) % b
        return rel, t % per

    def vis_blk(i, q, dx, dc, many):
        t = jnp.where(i < na + nb, jnp.minimum(i, na - 1), i - na - nb)
        here = ((q[0] + dx) % a) * b + (q[1] + dc) % b
        return (q[1] if many else 0, jnp.clip(t - here * per, 0, per - 1), 0, 0)

    own_in = pl.BlockSpec((1, n_own, pz, ny, nx), lambda i, q: (zblk(i, q)[0], 0, zblk(i, q)[1], 0, 0))
    vis_in = [
        pl.BlockSpec((1, pz, ny, nx), functools.partial(vis_blk, dx=r // b, dc=r % b, many=vis[r].shape[0] > 1))
        for r in range(a * b)
    ]
    prev_in = pl.BlockSpec((1, n_own, pz, ny, nx), lambda i, q: (zout(i, q)[0], 0, zout(i, q)[1], 0, 0))
    own_o = pl.BlockSpec((1, n_own, pz, ny, nx), lambda i, q: (zout(i, q)[0], 0, zout(i, q)[1], 0, 0))
    part_o = pl.BlockSpec((1, pz, ny, nx), lambda i, q: (zout(i, q)[0], zout(i, q)[1], 0, 0))
    tabs = [left_table(ny, False), left_table(ny, True), right_table(nx, False), right_table(nx, True), left_table(nz, False), left_table(nz, True)]
    tab_specs = [pl.BlockSpec(t.shape, lambda i, q: (0, 0), pipeline_mode=pl.Buffered(1)) for t in tabs]
    pitch = ny + pad
    body = functools.partial(fft_body, n=(nz, ny, nx), pz=pz, py=py, chunk=chunk, pitch=pitch, accumulate=prev is not None, n_own=n_own, four_pi=scale, pieces=pieces, zchunk=zchunk or chunk, lag=lag)
    ins = [own] + list(vis) + ([prev] if prev is not None else []) + [jnp.asarray(t) for t in tabs]
    specs = [own_in] + vis_in + ([prev_in] if prev is not None else []) + tab_specs
    flops = 6 * 3 * 2 * nz * ny * 4 * nx * nx
    return pl.pallas_call(
        body,
        grid_spec=pltpu.PrefetchScalarGridSpec(
            num_scalar_prefetch=1, grid=(2 * na + nb,), in_specs=specs, out_specs=[own_o, part_o],
            scratch_shapes=[pltpu.VMEM((nz * pitch, nx), F32), pltpu.VMEM((nz * pitch, nx), F32),
                            pltpu.VMEM((4 * max(ny, nz), max(pz, py) * nx), BF), pltpu.VMEM((pz * ny, 4 * nx), BF),
                            pltpu.VMEM((4 * nz, py * nx), BF), pltpu.VMEM((nz, nx), F32),
                            pltpu.VMEM((pz, ny, nx), F32)]),
        out_shape=[jax.ShapeDtypeStruct(own.shape, F32), jax.ShapeDtypeStruct((a * b, planes, ny, nx), F32)],
        compiler_params=pltpu.CompilerParams(vmem_limit_bytes=58 * 2**20),
        cost_estimate=pl.CostEstimate(flops=flops, bytes_accessed=64 * 2**20, transcendentals=0),
    )(q, *ins)


from jax.sharding import PartitionSpec as P

FRACTION = 0.25


def factors(size, own, vis):
    pairs = [(a, size // a) for a in range(1, size + 1) if size % a == 0]
    return min((p for p in pairs if own % p[0] == 0 and vis % p[1] == 0), key=lambda p: abs(p[0] - p[1]))


def from_slow(block, a, b, shift):
    if shift == 0:
        return block
    return lax.ppermute(block, "grid", [(((x + shift) % a) * b + c, x * b + c) for x in range(a) for c in range(b)])


def from_fast(block, a, b, shift):
    if shift == 0:
        return block
    return lax.ppermute(block, "grid", [(x * b + (c + shift) % b, x * b + c) for x in range(a) for c in range(b)])


def along_band(block, distance):
    size = lax.axis_size("band")
    return lax.ppermute(block, "band", [((i - distance) % size, i) for i in range(size)])


def body(own_bands, travel_bands):
    own_count, planes, ny, nx = own_bands.shape
    vis_count = travel_bands.shape[0]
    size = lax.axis_size("grid")
    a, b = factors(size, own_count, vis_count)
    n_own, n_vis = own_count // a, vis_count // b
    nz = planes * size
    index = lax.axis_index("grid")
    x, c = index // b, index % b
    q = jnp.stack([x, c]).astype(jnp.int32)
    scale = -FRACTION * 4.0 * math.pi / (nz * ny * nx)
    pz = math.gcd(planes, 16)
    py = math.gcd(ny, 32)

    def own_set(bands, s):
        return lax.dynamic_slice_in_dim(bands, s * n_own, n_own, 0)

    arrived = [along_band(travel_bands[:b], 1)]
    sent = [own_set(own_bands, (x - dx) % a) for dx in range(1, a)]
    sent, own_bands, travel_bands = lax.optimization_barrier((sent, own_bands, travel_bands))
    own_x = [from_slow(s, a, b, dx + 1) for dx, s in enumerate(sent)]
    for k in range(1, n_vis):
        arrived.append(along_band(travel_bands[k * b:(k + 1) * b], 1))
    own_x = [own_set(own_bands, x)] + own_x
    own_full = jnp.stack([from_fast(own_x[dx], a, b, dc) for dx in range(a) for dc in range(b)])

    groups = [(g, min(2, n_own - g)) for g in range(0, n_own, 2)]
    own_part = [None for _ in groups]
    returned = []
    last = None
    for k in range(n_vis):
        pieces = [from_slow(arrived[k], a, b, dx) for dx in range(a)]
        vis = []
        for dx in range(a):
            vis.append(pieces[dx])
            for dc in range(1, b):
                vis.append(from_fast(lax.dynamic_slice_in_dim(pieces[dx], (c - dc) % b, 1, 0), a, b, dc))
        partner = None
        for n, (g, w) in enumerate(groups):
            own_part[n], part = solve(q, own_full[:, g:g + w], vis, own_part[n], (a, b), scale, pz=pz, py=py)
            partner = part if partner is None else partner + part
        partner = partner.reshape(a, b, planes, ny, nx)
        back = []
        for dc in range(b):
            here = [from_fast(partner[dx, dc], a, b, (-dc) % b) for dx in range(a)]
            got = [from_slow(here[dx], a, b, (-dx) % a) for dx in range(1, a)]
            if last is not None:
                got, last = lax.optimization_barrier((got, last))
                if dc:
                    back[-1] = last
                else:
                    returned[-1][-1] = last
            last = here[0]
            for piece in got:
                last = last + piece
            back.append(last)
        returned.append(back)

    own_part = own_part[0] if len(groups) == 1 else jnp.concatenate(own_part, axis=1)
    own_part = own_part.reshape(a, b, n_own, planes, ny, nx)
    for dx in range(a):
        summed = own_part[dx, 0]
        for dc in range(1, b):
            summed = summed + from_fast(own_part[dx, dc], a, b, (-dc) % b)
        if dx == 0:
            own_out = jnp.concatenate([summed] * a, axis=0)
            continue
        got = from_slow(summed, a, b, (-dx) % a)
        own_out = lax.dynamic_update_slice_in_dim(own_out, got, ((x - dx) % a) * n_own, 0)
    partner_out = jnp.zeros_like(travel_bands)
    for k in range(n_vis):
        for dc in range(b):
            got = along_band(returned[k][dc], -1)
            partner_out = lax.dynamic_update_index_in_dim(partner_out, got, k * b + (c - dc) % b, 0)
    return own_out, partner_out


def solution(mesh):
    spec = P("band", "grid", None, None)
    return jax.shard_map(body, mesh=mesh, in_specs=(spec, spec), out_specs=(spec, spec), check_vma=False)
```

```python
import math, functools
import numpy as np
import jax
import jax.numpy as jnp
from jax import lax
from jax.experimental import pallas as pl
from jax.experimental.pallas import tpu as pltpu
import ml_dtypes
BF = jnp.bfloat16
F32 = jnp.float32


def split_table(t):
    hi = t.astype(np.float32).astype(ml_dtypes.bfloat16)
    lo = (t - hi.astype(np.float64)).astype(np.float32).astype(ml_dtypes.bfloat16)
    return hi, lo


def dft(length, inverse):
    k = np.arange(length)
    ang = 2.0 * np.pi / length * ((k[:, None] * k[None, :]) % length)
    c, s = np.cos(ang), np.sin(ang)
    if inverse:
        s = -s
    return np.block([[c, s], [-s, c]])


def left_table(length, inverse):
    hi, lo = split_table(dft(length, inverse))
    return np.concatenate([hi, hi, lo], axis=1)


def right_table(length, inverse):
    hi, lo = split_table(dft(length, inverse).T)
    return np.concatenate([hi, hi, lo], axis=0)


def parts(v):
    hi = v.astype(BF)
    lo = (v - hi.astype(F32)).astype(BF)
    return hi, lo


def fft_body(*refs, n, pz, py, chunk, pitch, accumulate, n_own, four_pi, pieces, zchunk, lag):
    nz, ny, nx = n
    q_ref, own_ref = refs[:2]
    a, b = pieces
    vis_refs = refs[2:2 + a * b]
    rest = list(refs[2 + a * b:])
    prev_ref = rest.pop(0) if accumulate else None
    lyf, lyi, rxf, rxi, lzf, lzi, own_out = rest[:7]
    part_outs = rest[7:7 + a * b]
    re_s, im_s, st_l, st_r, st_z2, ksq, vis_ref = rest[7 + a * b:]
    st_z = st_l
    step = pl.program_id(0)
    na = nz // pz
    nb = ny // py

    def put_left(st, a, j, w, re, im):
        rh, rl = parts(re); ih, il = parts(im)
        col = slice(j * w, (j + 1) * w)
        st[0 * a:1 * a, col] = rh
        st[1 * a:2 * a, col] = ih
        st[2 * a:3 * a, col] = rl
        st[3 * a:4 * a, col] = il

    def put_right(st, a, w, j, re, im):
        rh, rl = parts(re); ih, il = parts(im)
        row = slice(j * a, (j + 1) * a)
        st[row, 0 * w:1 * w] = rh
        st[row, 1 * w:2 * w] = ih
        st[row, 2 * w:3 * w] = rl
        st[row, 3 * w:4 * w] = il

    def left(st, a, lo, hi):
        return jnp.concatenate([st[:4 * a, lo:hi], st[:2 * a, lo:hi]], axis=0)

    def right(st, w, lo, hi):
        return jnp.concatenate([st[lo:hi, :], st[lo:hi, :2 * w]], axis=1)

    def dot(a, b):
        return lax.dot_general(a, b, (((1,), (0,)), ((), ())), preferred_element_type=F32)

    def pipeline(first, second, third, count, width):
        n = count // width
        for t in range(n + 2 * lag):
            if t < n:
                first(t * width)
            if 0 <= t - lag < n:
                second((t - lag) * width)
            if 0 <= t - 2 * lag < n:
                third((t - 2 * lag) * width)

    plane = jnp.where(step < na, step, step - na - nb)
    natural = plane // (na // (a * b))
    for dx in range(a):
        for dc in range(b):
            here = ((q_ref[0] + dx) % a) * b + (q_ref[1] + dc) % b

            @pl.when(((step < na) | (step >= na + nb)) & (natural == here))
            def _(dx=dx, dc=dc):
                vis_ref[...] = vis_refs[dx * b + dc][0]

    @pl.when(step < na)
    def _():
        z0 = step * pz

        def density(c0):
            for p in range(c0, c0 + chunk):
                v = vis_ref[p]
                re = own_ref[0, 0, p] * v
                im = own_ref[0, 1, p] * v if n_own == 2 else jnp.zeros_like(re)
                put_left(st_l, ny, p, nx, re, im)

        def yforward(c0):
            y1 = dot(lyf[...], left(st_l, ny, c0 * nx, (c0 + chunk) * nx))
            for p in range(c0, c0 + chunk):
                j = p - c0
                put_right(st_r, ny, nx, p, y1[:ny, j * nx:(j + 1) * nx], y1[ny:, j * nx:(j + 1) * nx])

        def xforward(c0):
            y2 = dot(right(st_r, nx, c0 * ny, (c0 + chunk) * ny), rxf[...])
            for p in range(c0, c0 + chunk):
                j = p - c0
                row = pl.multiple_of((z0 + p) * pitch, 8)
                re_s[pl.ds(row, ny), :] = y2[j * ny:(j + 1) * ny, :nx]
                im_s[pl.ds(row, ny), :] = y2[j * ny:(j + 1) * ny, nx:]

        pipeline(density, yforward, xforward, pz, chunk)

    def square(i, length):
        pos = jnp.where(i >= length // 2, i - length, i).astype(F32) * F32(2.0 * math.pi / length)
        return pos * pos

    @pl.when(step == na)
    def _():
        iz = lax.broadcasted_iota(jnp.int32, (nz, nx), 0)
        ix = lax.broadcasted_iota(jnp.int32, (nz, nx), 1)
        ksq[...] = square(iz, nz) + square(ix, nx)

    @pl.when((step >= na) & (step < na + nb))
    def _():
        y0 = (step - na) * py

        def zload(c0):
            for j in range(c0, c0 + zchunk):
                re = re_s[pl.ds(y0 + j, nz, stride=pitch), :]
                im = im_s[pl.ds(y0 + j, nz, stride=pitch), :]
                put_left(st_z, nz, j, nx, re, im)

        def zforward(c0):
            f = dot(lzf[...], left(st_z, nz, c0 * nx, (c0 + zchunk) * nx))
            for j in range(c0, c0 + zchunk):
                k2 = ksq[...] + square(y0 + j, ny)
                kern = jnp.where(k2 > 0.0, F32(four_pi) / jnp.where(k2 > 0.0, k2, 1.0), 0.0)
                i = j - c0
                put_left(st_z2, nz, j, nx, f[:nz, i * nx:(i + 1) * nx] * kern, f[nz:, i * nx:(i + 1) * nx] * kern)

        def zinverse(c0):
            g = dot(lzi[...], left(st_z2, nz, c0 * nx, (c0 + zchunk) * nx))
            for j in range(c0, c0 + zchunk):
                i = j - c0
                re_s[pl.ds(y0 + j, nz, stride=pitch), :] = g[:nz, i * nx:(i + 1) * nx]
                im_s[pl.ds(y0 + j, nz, stride=pitch), :] = g[nz:, i * nx:(i + 1) * nx]

        pipeline(zload, zforward, zinverse, py, zchunk)

    @pl.when(step >= na + nb)
    def _():
        z0 = (step - na - nb) * pz

        def spectrum(c0):
            for p in range(c0, c0 + chunk):
                row = pl.multiple_of((z0 + p) * pitch, 8)
                put_right(st_r, ny, nx, p, re_s[pl.ds(row, ny), :], im_s[pl.ds(row, ny), :])

        def xinverse(c0):
            y2 = dot(right(st_r, nx, c0 * ny, (c0 + chunk) * ny), rxi[...])
            for p in range(c0, c0 + chunk):
                j = p - c0
                put_left(st_l, ny, p, nx, y2[j * ny:(j + 1) * ny, :nx], y2[j * ny:(j + 1) * ny, nx:])

        def yinverse(c0):
            y1 = dot(lyi[...], left(st_l, ny, c0 * nx, (c0 + chunk) * nx))
            for p in range(c0, c0 + chunk):
                j = p - c0
                v = vis_ref[p]
                va = y1[:ny, j * nx:(j + 1) * nx]
                o = va * v
                own_out[0, 0, p] = o + prev_ref[0, 0, p] if accumulate else o
                pt = va * own_ref[0, 0, p]
                if n_own == 2:
                    vb = y1[ny:, j * nx:(j + 1) * nx]
                    o = vb * v
                    own_out[0, 1, p] = o + prev_ref[0, 1, p] if accumulate else o
                    pt = pt + vb * own_ref[0, 1, p]
                vis_ref[p] = pt

        pipeline(spectrum, xinverse, yinverse, pz, chunk)
        for dx in range(a):
            for dc in range(b):
                here = ((q_ref[0] + dx) % a) * b + (q_ref[1] + dc) % b

                @pl.when(natural == here)
                def _(dx=dx, dc=dc):
                    part_outs[dx * b + dc][...] = vis_ref[...]


def solve(q, own, vis, prev, pieces, scale, pz=8, py=8, chunk=2, pad=8, zchunk=None, lag=1):
    _, n_own, planes, ny, nx = own.shape
    a, b = pieces
    nz = planes * a * b
    na, nb = nz // pz, ny // py
    per = planes // pz

    def zblk(i, q):
        t = jnp.where(i < na, i, jnp.maximum(i - nb, na) - na)
        t = jnp.where((i >= na) & (i < na + nb), na - 1, t)
        piece = t // per
        x, c = piece // b, piece % b
        rel = ((x - q[0] + a) % a) * b + (c - q[1] + b) % b
        return rel, t % per

    def zout(i, q):
        t = jnp.maximum(i - nb - na, 0)
        piece = t // per
        x, c = piece // b, piece % b
        rel = ((x - q[0] + a) % a) * b + (c - q[1] + b) % b
        return rel, t % per

    def vis_blk(i, q, dx, dc, many):
        t = jnp.where(i < na + nb, jnp.minimum(i, na - 1), i - na - nb)
        here = ((q[0] + dx) % a) * b + (q[1] + dc) % b
        return (q[1] if many else 0, jnp.clip(t - here * per, 0, per - 1), 0, 0)

    own_in = pl.BlockSpec((1, n_own, pz, ny, nx), lambda i, q: (zblk(i, q)[0], 0, zblk(i, q)[1], 0, 0))
    vis_in = [
        pl.BlockSpec((1, pz, ny, nx), functools.partial(vis_blk, dx=r // b, dc=r % b, many=vis[r].shape[0] > 1))
        for r in range(a * b)
    ]
    prev_in = pl.BlockSpec((1, n_own, pz, ny, nx), lambda i, q: (zout(i, q)[0], 0, zout(i, q)[1], 0, 0))
    own_o = pl.BlockSpec((1, n_own, pz, ny, nx), lambda i, q: (zout(i, q)[0], 0, zout(i, q)[1], 0, 0))

    def part_blk(i, q, dx, dc):
        here = ((q[0] + dx) % a) * b + (q[1] + dc) % b
        return (jnp.clip(i - na - nb - here * per, 0, per - 1), 0, 0)

    part_o = [pl.BlockSpec((pz, ny, nx), functools.partial(part_blk, dx=r // b, dc=r % b)) for r in range(a * b)]
    tabs = [left_table(ny, False), left_table(ny, True), right_table(nx, False), right_table(nx, True), left_table(nz, False), left_table(nz, True)]
    tab_specs = [pl.BlockSpec(t.shape, lambda i, q: (0, 0), pipeline_mode=pl.Buffered(1)) for t in tabs]
    pitch = ny + pad
    body = functools.partial(fft_body, n=(nz, ny, nx), pz=pz, py=py, chunk=chunk, pitch=pitch, accumulate=prev is not None, n_own=n_own, four_pi=scale, pieces=pieces, zchunk=zchunk or chunk, lag=lag)
    ins = [own] + list(vis) + ([prev] if prev is not None else []) + [jnp.asarray(t) for t in tabs]
    specs = [own_in] + vis_in + ([prev_in] if prev is not None else []) + tab_specs
    flops = 6 * 3 * 2 * nz * ny * 4 * nx * nx
    return pl.pallas_call(
        body,
        grid_spec=pltpu.PrefetchScalarGridSpec(
            num_scalar_prefetch=1, grid=(2 * na + nb,), in_specs=specs, out_specs=[own_o] + part_o,
            scratch_shapes=[pltpu.VMEM((nz * pitch, nx), F32), pltpu.VMEM((nz * pitch, nx), F32),
                            pltpu.VMEM((4 * max(ny, nz), max(pz, py) * nx), BF), pltpu.VMEM((pz * ny, 4 * nx), BF),
                            pltpu.VMEM((4 * nz, py * nx), BF), pltpu.VMEM((nz, nx), F32),
                            pltpu.VMEM((pz, ny, nx), F32)]),
        out_shape=[jax.ShapeDtypeStruct(own.shape, F32), *[jax.ShapeDtypeStruct((planes, ny, nx), F32)] * (a * b)],
        compiler_params=pltpu.CompilerParams(vmem_limit_bytes=60 * 2**20),
        cost_estimate=pl.CostEstimate(flops=flops, bytes_accessed=64 * 2**20, transcendentals=0),
    )(q, *ins)


from jax.sharding import PartitionSpec as P

FRACTION = 0.25


def factors(size, own, vis):
    pairs = [(a, size // a) for a in range(1, size + 1) if size % a == 0]
    return min((p for p in pairs if own % p[0] == 0 and vis % p[1] == 0), key=lambda p: abs(p[0] - p[1]))


def from_slow(block, a, b, shift):
    if shift == 0:
        return block
    return lax.ppermute(block, "grid", [(((x + shift) % a) * b + c, x * b + c) for x in range(a) for c in range(b)])


def from_fast(block, a, b, shift):
    if shift == 0:
        return block
    return lax.ppermute(block, "grid", [(x * b + (c + shift) % b, x * b + c) for x in range(a) for c in range(b)])


def along_band(block, distance):
    size = lax.axis_size("band")
    return lax.ppermute(block, "band", [((i - distance) % size, i) for i in range(size)])


def body(own_bands, travel_bands):
    own_count, planes, ny, nx = own_bands.shape
    vis_count = travel_bands.shape[0]
    size = lax.axis_size("grid")
    a, b = factors(size, own_count, vis_count)
    n_own, n_vis = own_count // a, vis_count // b
    nz = planes * size
    index = lax.axis_index("grid")
    x, c = index // b, index % b
    q = jnp.stack([x, c]).astype(jnp.int32)
    scale = -FRACTION * 4.0 * math.pi / (nz * ny * nx)
    pz = math.gcd(planes, 16)
    py = math.gcd(ny, max(8, ny // size))

    def own_set(bands, s):
        return lax.dynamic_slice_in_dim(bands, s * n_own, n_own, 0)

    arrived = [along_band(travel_bands[:b], 1)]
    sent = [own_set(own_bands, (x - dx) % a) for dx in range(1, a)]
    sent, own_bands, travel_bands = lax.optimization_barrier((sent, own_bands, travel_bands))
    own_x = [from_slow(s, a, b, dx + 1) for dx, s in enumerate(sent)]
    for k in range(1, n_vis):
        arrived.append(along_band(travel_bands[k * b:(k + 1) * b], 1))
    own_x = [own_set(own_bands, x)] + own_x
    own_full = jnp.stack([from_fast(own_x[dx], a, b, dc) for dx in range(a) for dc in range(b)])

    groups = [(g, min(2, n_own - g)) for g in range(0, n_own, 2)]
    own_part = [None for _ in groups]
    returned = []
    last = None
    for k in range(n_vis):
        pieces = [from_slow(arrived[k], a, b, dx) for dx in range(a)]
        vis = []
        for dx in range(a):
            vis.append(pieces[dx])
            for dc in range(1, b):
                vis.append(from_fast(lax.dynamic_slice_in_dim(pieces[dx], (c - dc) % b, 1, 0), a, b, dc))
        partner = None
        for n, (g, w) in enumerate(groups):
            own_part[n], *part = solve(q, own_full[:, g:g + w], vis, own_part[n], (a, b), scale, pz=pz, py=py)
            partner = part if partner is None else [p + r for p, r in zip(partner, part)]
        back = []
        for dc in range(b):
            here = [from_fast(partner[dx * b + dc], a, b, (-dc) % b) for dx in range(a)]
            got = [from_slow(here[dx], a, b, (-dx) % a) for dx in range(1, a)]
            if last is not None:
                got, _ = lax.optimization_barrier((got, last))
            last = here[0]
            for piece in got:
                last = last + piece
            back.append(last)
        returned.append(back)

    own_part = own_part[0] if len(groups) == 1 else jnp.concatenate(own_part, axis=1)
    own_part = own_part.reshape(a, b, n_own, planes, ny, nx)
    for dx in range(a):
        summed = own_part[dx, 0]
        for dc in range(1, b):
            summed = summed + from_fast(own_part[dx, dc], a, b, (-dc) % b)
        if dx == 0:
            own_out = jnp.concatenate([summed] * a, axis=0)
            continue
        got = from_slow(summed, a, b, (-dx) % a)
        own_out = lax.dynamic_update_slice_in_dim(own_out, got, ((x - dx) % a) * n_own, 0)
    partner_out = jnp.zeros_like(travel_bands)
    for k in range(n_vis):
        for dc in range(b):
            got = along_band(returned[k][dc], -1)
            partner_out = lax.dynamic_update_index_in_dim(partner_out, got, k * b + (c - dc) % b, 0)
    return own_out, partner_out


def solution(mesh):
    spec = P("band", "grid", None, None)
    return jax.shard_map(body, mesh=mesh, in_specs=(spec, spec), out_specs=(spec, spec), check_vma=False)
```

```python
import math, functools
import numpy as np
import jax
import jax.numpy as jnp
from jax import lax
from jax.experimental import pallas as pl
from jax.experimental.pallas import tpu as pltpu
import ml_dtypes
BF = jnp.bfloat16
F32 = jnp.float32


def split_table(t):
    hi = t.astype(np.float32).astype(ml_dtypes.bfloat16)
    lo = (t - hi.astype(np.float64)).astype(np.float32).astype(ml_dtypes.bfloat16)
    return hi, lo


def dft(length, inverse):
    k = np.arange(length)
    ang = 2.0 * np.pi / length * ((k[:, None] * k[None, :]) % length)
    c, s = np.cos(ang), np.sin(ang)
    if inverse:
        s = -s
    return np.block([[c, s], [-s, c]])


def left_table(length, inverse):
    hi, lo = split_table(dft(length, inverse))
    return np.concatenate([hi, hi, lo], axis=1)


def right_table(length, inverse):
    hi, lo = split_table(dft(length, inverse).T)
    return np.concatenate([hi, hi, lo], axis=0)


def parts(v):
    hi = v.astype(BF)
    lo = (v - hi.astype(F32)).astype(BF)
    return hi, lo


def fft_body(*refs, n, pz, py, chunk, pitch, accumulate, n_own, four_pi, pieces, zchunk, lag):
    nz, ny, nx = n
    q_ref, own_ref = refs[:2]
    a, b = pieces
    vis_refs = refs[2:2 + a * b]
    rest = list(refs[2 + a * b:])
    prev_ref = rest.pop(0) if accumulate else None
    lyf, lyi, rxf, rxi, lzf, lzi, own_out = rest[:7]
    part_outs = rest[7:7 + a * b]
    re_s, im_s, st_l, st_r, st_z2, ksq, vis_ref = rest[7 + a * b:]
    st_z = st_l
    step = pl.program_id(0)
    na = nz // pz
    nb = ny // py

    def put_left(st, a, j, w, re, im):
        rh, rl = parts(re); ih, il = parts(im)
        col = slice(j * w, (j + 1) * w)
        st[0 * a:1 * a, col] = rh
        st[1 * a:2 * a, col] = ih
        st[2 * a:3 * a, col] = rl
        st[3 * a:4 * a, col] = il

    def put_right(st, a, w, j, re, im):
        rh, rl = parts(re); ih, il = parts(im)
        row = slice(j * a, (j + 1) * a)
        st[row, 0 * w:1 * w] = rh
        st[row, 1 * w:2 * w] = ih
        st[row, 2 * w:3 * w] = rl
        st[row, 3 * w:4 * w] = il

    def left(st, a, lo, hi):
        return jnp.concatenate([st[:4 * a, lo:hi], st[:2 * a, lo:hi]], axis=0)

    def right(st, w, lo, hi):
        return jnp.concatenate([st[lo:hi, :], st[lo:hi, :2 * w]], axis=1)

    def dot(a, b):
        return lax.dot_general(a, b, (((1,), (0,)), ((), ())), preferred_element_type=F32)

    def pipeline(first, second, third, count, width):
        n = count // width
        for t in range(n + 2 * lag):
            if t < n:
                first(t * width)
            if 0 <= t - lag < n:
                second((t - lag) * width)
            if 0 <= t - 2 * lag < n:
                third((t - 2 * lag) * width)

    plane = jnp.where(step < na, step, step - na - nb)
    natural = plane // (na // (a * b))
    for dx in range(a):
        for dc in range(b):
            here = ((q_ref[0] + dx) % a) * b + (q_ref[1] + dc) % b

            @pl.when(((step < na) | (step >= na + nb)) & (natural == here))
            def _(dx=dx, dc=dc):
                vis_ref[...] = vis_refs[dx * b + dc][0]

    @pl.when(step < na)
    def _():
        z0 = step * pz

        def density(c0):
            for p in range(c0, c0 + chunk):
                v = vis_ref[p]
                re = own_ref[0, 0, p] * v
                im = own_ref[0, 1, p] * v if n_own == 2 else jnp.zeros_like(re)
                put_left(st_l, ny, p, nx, re, im)

        def yforward(c0):
            y1 = dot(lyf[...], left(st_l, ny, c0 * nx, (c0 + chunk) * nx))
            for p in range(c0, c0 + chunk):
                j = p - c0
                put_right(st_r, ny, nx, p, y1[:ny, j * nx:(j + 1) * nx], y1[ny:, j * nx:(j + 1) * nx])

        def xforward(c0):
            y2 = dot(right(st_r, nx, c0 * ny, (c0 + chunk) * ny), rxf[...])
            for p in range(c0, c0 + chunk):
                j = p - c0
                row = pl.multiple_of((z0 + p) * pitch, 8)
                re_s[pl.ds(row, ny), :] = y2[j * ny:(j + 1) * ny, :nx]
                im_s[pl.ds(row, ny), :] = y2[j * ny:(j + 1) * ny, nx:]

        pipeline(density, yforward, xforward, pz, chunk)

    def square(i, length):
        pos = jnp.where(i >= length // 2, i - length, i).astype(F32) * F32(2.0 * math.pi / length)
        return pos * pos

    @pl.when(step == na)
    def _():
        iz = lax.broadcasted_iota(jnp.int32, (nz, nx), 0)
        ix = lax.broadcasted_iota(jnp.int32, (nz, nx), 1)
        ksq[...] = square(iz, nz) + square(ix, nx)

    @pl.when((step >= na) & (step < na + nb))
    def _():
        y0 = (step - na) * py

        def zload(c0):
            for j in range(c0, c0 + zchunk):
                re = re_s[pl.ds(y0 + j, nz, stride=pitch), :]
                im = im_s[pl.ds(y0 + j, nz, stride=pitch), :]
                put_left(st_z, nz, j, nx, re, im)

        def zforward(c0):
            f = dot(lzf[...], left(st_z, nz, c0 * nx, (c0 + zchunk) * nx))
            for j in range(c0, c0 + zchunk):
                k2 = ksq[...] + square(y0 + j, ny)
                kern = jnp.where(k2 > 0.0, F32(four_pi) / jnp.where(k2 > 0.0, k2, 1.0), 0.0)
                i = j - c0
                put_left(st_z2, nz, j, nx, f[:nz, i * nx:(i + 1) * nx] * kern, f[nz:, i * nx:(i + 1) * nx] * kern)

        def zinverse(c0):
            g = dot(lzi[...], left(st_z2, nz, c0 * nx, (c0 + zchunk) * nx))
            for j in range(c0, c0 + zchunk):
                i = j - c0
                re_s[pl.ds(y0 + j, nz, stride=pitch), :] = g[:nz, i * nx:(i + 1) * nx]
                im_s[pl.ds(y0 + j, nz, stride=pitch), :] = g[nz:, i * nx:(i + 1) * nx]

        pipeline(zload, zforward, zinverse, py, zchunk)

    @pl.when(step >= na + nb)
    def _():
        z0 = (step - na - nb) * pz

        def spectrum(c0):
            for p in range(c0, c0 + chunk):
                row = pl.multiple_of((z0 + p) * pitch, 8)
                put_right(st_r, ny, nx, p, re_s[pl.ds(row, ny), :], im_s[pl.ds(row, ny), :])

        def xinverse(c0):
            y2 = dot(right(st_r, nx, c0 * ny, (c0 + chunk) * ny), rxi[...])
            for p in range(c0, c0 + chunk):
                j = p - c0
                put_left(st_l, ny, p, nx, y2[j * ny:(j + 1) * ny, :nx], y2[j * ny:(j + 1) * ny, nx:])

        def yinverse(c0):
            y1 = dot(lyi[...], left(st_l, ny, c0 * nx, (c0 + chunk) * nx))
            for p in range(c0, c0 + chunk):
                j = p - c0
                v = vis_ref[p]
                va = y1[:ny, j * nx:(j + 1) * nx]
                o = va * v
                own_out[0, 0, p] = o + prev_ref[0, 0, p] if accumulate else o
                pt = va * own_ref[0, 0, p]
                if n_own == 2:
                    vb = y1[ny:, j * nx:(j + 1) * nx]
                    o = vb * v
                    own_out[0, 1, p] = o + prev_ref[0, 1, p] if accumulate else o
                    pt = pt + vb * own_ref[0, 1, p]
                vis_ref[p] = pt

        pipeline(spectrum, xinverse, yinverse, pz, chunk)
        for dx in range(a):
            for dc in range(b):
                here = ((q_ref[0] + dx) % a) * b + (q_ref[1] + dc) % b

                @pl.when(natural == here)
                def _(dx=dx, dc=dc):
                    part_outs[dx * b + dc][...] = vis_ref[...]


def solve(q, own, vis, prev, pieces, scale, pz=8, py=8, chunk=2, pad=8, zchunk=None, lag=1):
    _, n_own, planes, ny, nx = own.shape
    a, b = pieces
    nz = planes * a * b
    na, nb = nz // pz, ny // py
    per = planes // pz

    def zblk(i, q):
        t = jnp.where(i < na, i, jnp.maximum(i - nb, na) - na)
        t = jnp.where((i >= na) & (i < na + nb), na - 1, t)
        piece = t // per
        x, c = piece // b, piece % b
        rel = ((x - q[0] + a) % a) * b + (c - q[1] + b) % b
        return rel, t % per

    def zout(i, q):
        t = jnp.maximum(i - nb - na, 0)
        piece = t // per
        x, c = piece // b, piece % b
        rel = ((x - q[0] + a) % a) * b + (c - q[1] + b) % b
        return rel, t % per

    def vis_blk(i, q, dx, dc, many):
        t = jnp.where(i < na + nb, jnp.minimum(i, na - 1), i - na - nb)
        here = ((q[0] + dx) % a) * b + (q[1] + dc) % b
        return (q[1] if many else 0, jnp.clip(t - here * per, 0, per - 1), 0, 0)

    own_in = pl.BlockSpec((1, n_own, pz, ny, nx), lambda i, q: (zblk(i, q)[0], 0, zblk(i, q)[1], 0, 0))
    vis_in = [
        pl.BlockSpec((1, pz, ny, nx), functools.partial(vis_blk, dx=r // b, dc=r % b, many=vis[r].shape[0] > 1))
        for r in range(a * b)
    ]
    prev_in = pl.BlockSpec((1, n_own, pz, ny, nx), lambda i, q: (zout(i, q)[0], 0, zout(i, q)[1], 0, 0))
    own_o = pl.BlockSpec((1, n_own, pz, ny, nx), lambda i, q: (zout(i, q)[0], 0, zout(i, q)[1], 0, 0))

    def part_blk(i, q, dx, dc):
        here = ((q[0] + dx) % a) * b + (q[1] + dc) % b
        return (jnp.clip(i - na - nb - here * per, 0, per - 1), 0, 0)

    part_o = [pl.BlockSpec((pz, ny, nx), functools.partial(part_blk, dx=r // b, dc=r % b)) for r in range(a * b)]
    tabs = [left_table(ny, False), left_table(ny, True), right_table(nx, False), right_table(nx, True), left_table(nz, False), left_table(nz, True)]
    tab_specs = [pl.BlockSpec(t.shape, lambda i, q: (0, 0), pipeline_mode=pl.Buffered(1)) for t in tabs]
    pitch = ny + pad
    body = functools.partial(fft_body, n=(nz, ny, nx), pz=pz, py=py, chunk=chunk, pitch=pitch, accumulate=prev is not None, n_own=n_own, four_pi=scale, pieces=pieces, zchunk=zchunk or chunk, lag=lag)
    ins = [own] + list(vis) + ([prev] if prev is not None else []) + [jnp.asarray(t) for t in tabs]
    specs = [own_in] + vis_in + ([prev_in] if prev is not None else []) + tab_specs
    flops = 6 * 3 * 2 * nz * ny * 4 * nx * nx
    return pl.pallas_call(
        body,
        grid_spec=pltpu.PrefetchScalarGridSpec(
            num_scalar_prefetch=1, grid=(2 * na + nb,), in_specs=specs, out_specs=[own_o] + part_o,
            scratch_shapes=[pltpu.VMEM((nz * pitch, nx), F32), pltpu.VMEM((nz * pitch, nx), F32),
                            pltpu.VMEM((4 * max(ny, nz), max(pz, py) * nx), BF), pltpu.VMEM((pz * ny, 4 * nx), BF),
                            pltpu.VMEM((4 * nz, py * nx), BF), pltpu.VMEM((nz, nx), F32),
                            pltpu.VMEM((pz, ny, nx), F32)]),
        out_shape=[jax.ShapeDtypeStruct(own.shape, F32), *[jax.ShapeDtypeStruct((planes, ny, nx), F32)] * (a * b)],
        compiler_params=pltpu.CompilerParams(vmem_limit_bytes=60 * 2**20),
        cost_estimate=pl.CostEstimate(flops=flops, bytes_accessed=64 * 2**20, transcendentals=0),
    )(q, *ins)


from jax.sharding import PartitionSpec as P

FRACTION = 0.25


def factors(size, own, vis):
    pairs = [(a, size // a) for a in range(1, size + 1) if size % a == 0]
    return min((p for p in pairs if own % p[0] == 0 and vis % p[1] == 0), key=lambda p: abs(p[0] - p[1]))


def from_slow(block, a, b, shift):
    if shift == 0:
        return block
    return lax.ppermute(block, "grid", [(((x + shift) % a) * b + c, x * b + c) for x in range(a) for c in range(b)])


def from_fast(block, a, b, shift):
    if shift == 0:
        return block
    return lax.ppermute(block, "grid", [(x * b + (c + shift) % b, x * b + c) for x in range(a) for c in range(b)])


def along_band(block, distance):
    size = lax.axis_size("band")
    return lax.ppermute(block, "band", [((i - distance) % size, i) for i in range(size)])


def body(own_bands, travel_bands):
    own_count, planes, ny, nx = own_bands.shape
    vis_count = travel_bands.shape[0]
    size = lax.axis_size("grid")
    a, b = factors(size, own_count, vis_count)
    n_own, n_vis = own_count // a, vis_count // b
    nz = planes * size
    index = lax.axis_index("grid")
    x, c = index // b, index % b
    q = jnp.stack([x, c]).astype(jnp.int32)
    scale = -FRACTION * 4.0 * math.pi / (nz * ny * nx)
    pz = math.gcd(planes, 16)
    py = math.gcd(ny, max(8, ny // size))

    def own_set(bands, s):
        return lax.dynamic_slice_in_dim(bands, s * n_own, n_own, 0)

    arrived = [along_band(travel_bands[:b], 1)]
    sent = [own_set(own_bands, (x - dx) % a) for dx in range(1, a)]
    sent, own_bands, travel_bands = lax.optimization_barrier((sent, own_bands, travel_bands))
    own_x = [from_slow(s, a, b, dx + 1) for dx, s in enumerate(sent)]
    for k in range(1, n_vis):
        arrived.append(along_band(travel_bands[k * b:(k + 1) * b], 1))
    own_x = [own_set(own_bands, x)] + own_x
    own_full = jnp.stack([from_fast(own_x[dx], a, b, dc) for dx in range(a) for dc in range(b)])

    groups = [(g, min(2, n_own - g)) for g in range(0, n_own, 2)]
    own_part = [None for _ in groups]
    returned = []
    last = None
    for k in range(n_vis):
        pieces = [from_slow(arrived[k], a, b, dx) for dx in range(a)]
        vis = []
        for dx in range(a):
            vis.append(pieces[dx])
            for dc in range(1, b):
                vis.append(from_fast(lax.dynamic_slice_in_dim(pieces[dx], (c - dc) % b, 1, 0), a, b, dc))
        partner = None
        for n, (g, w) in enumerate(groups):
            own_part[n], *part = solve(q, own_full[:, g:g + w], vis, own_part[n], (a, b), scale, pz=pz, py=py)
            partner = part if partner is None else [p + r for p, r in zip(partner, part)]
        back = []
        for dc in range(b):
            here = [from_fast(partner[dx * b + dc], a, b, (-dc) % b) for dx in range(a)]
            got = [from_slow(here[dx], a, b, (-dx) % a) for dx in range(1, a)]
            if last is not None:
                got, _ = lax.optimization_barrier((got, last))
            last = here[0]
            for piece in got:
                last = last + piece
            back.append(last)
        returned.append(back)

    own_part = own_part[0] if len(groups) == 1 else jnp.concatenate(own_part, axis=1)
    own_part = own_part.reshape(a, b, n_own, planes, ny, nx)
    for dx in range(a):
        summed = own_part[dx, 0]
        for dc in range(1, b):
            summed = summed + from_fast(own_part[dx, dc], a, b, (-dc) % b)
        if dx == 0:
            own_out = jnp.concatenate([summed] * a, axis=0)
            continue
        for i in range(n_own):
            got = from_slow(summed[i:i + 1], a, b, (-dx) % a)
            own_out = lax.dynamic_update_slice_in_dim(own_out, got, ((x - dx) % a) * n_own + i, 0)
    partner_out = jnp.zeros_like(travel_bands)
    for k in range(n_vis):
        for dc in range(b):
            got = along_band(returned[k][dc], -1)
            partner_out = lax.dynamic_update_index_in_dim(partner_out, got, k * b + (c - dc) % b, 0)
    return own_out, partner_out


def solution(mesh):
    spec = P("band", "grid", None, None)
    return jax.shard_map(body, mesh=mesh, in_specs=(spec, spec), out_specs=(spec, spec), check_vma=False)
```
